128 devices in a mesh: row: 8 (over x, z_lo), col: 16 (over z_hi, y, core).
Axes of the slice: x: 4, y: 4, z: 4 (z_hi: 2, z_lo: 2; z = z_hi * 2 + z_lo), core: 2. Of those that a mesh axis runs over, the one named last changes fastest.
Arguments:
- slab: bfloat16 [1024, 128, 128], P(('row', 'col')), may hold values from -6 to 6
- pair: bfloat16 [1024, 1024, 128], P('row', 'col'), may hold values from -6 to 6
- mask: int32 [1024], replicated, may hold values 0 or 1
- ln_gain: float32 [128], replicated, may hold values from 0.1 to 1.9
- w_query: bfloat16 [128, 128], replicated, may hold values from -0.5 to 0.5
- w_key: bfloat16 [128, 128], replicated, may hold values from -0.5 to 0.5
- w_value: bfloat16 [128, 128], replicated, may hold values from -0.5 to 0.5
- w_gate: bfloat16 [128, 128], replicated, may hold values from -0.5 to 0.5
- gate_bias: float32 [128], replicated, may hold values from -4 to 4
- w_bias: bfloat16 [128, 4], replicated, may hold values from -24 to 24
- w_out: bfloat16 [128, 128], replicated, may hold values from -0.5 to 0.5
- out_bias: float32 [128], replicated, may hold values from -3 to 3
Outputs:
- update: bfloat16 [1024, 128, 128], P(('row', 'col'))
The draws below stay inside these ranges and needn't reach their ends.
Inputs may be any that keep to these rules, and one draw needn't show every extreme that they name: `mask`: 1 marks a real token, 0 a padding token.
All inputs are finite; a program needn't handle non-finite values.
Results may differ from the reference program's by a relative error of at most 0.01.
The reference program's roundings to bfloat16 on the way (of `tri_bias`, `weights` and `hidden`) count: a program that leaves them out, or rounds other values in their place, can miss the bound.
Values may be sent and summed in bfloat16 or wider, within the bound.
No kernel may reach another device: no remote copies, remote signals or barrier semaphores. Data moves between devices by JAX's collectives and lax.ppermute only.
A program may use at most 128 MiB of HBM per device.

```python
import math
import jax
import jax.numpy as jnp
from jax import lax

TOK_BLK = 8
SLAB = 128
C = 128
H = 4
DH = 32
N = 1024
N_ROW = 8
N_COL = 16


def draw_w_bias(key, part):
    raw = jax.random.normal(key, (C, H), jnp.float32)
    values = jnp.clip(raw / math.sqrt(C), -24.0, 24.0)
    return values.astype(jnp.bfloat16)


def place_ends(array, rng, low, high):
    place = [jax.random.randint(jax.random.fold_in(rng, axis), (), 0, length) for axis, length in enumerate(array.shape)]
    main_axis = array.shape.index(max(array.shape))
    neighbour = place[:main_axis] + [(place[main_axis] + 1) % array.shape[main_axis]] + place[main_axis + 1:]
    return array.at[tuple(place)].set(low).at[tuple(neighbour)].set(high)


def levels(own_key, extent, split, least, high):
    level = 1.0
    for position, blocks in split:
        steps = jax.random.uniform(jax.random.fold_in(jax.random.fold_in(own_key, 6), position), (blocks,), jnp.float32, least / len(split), high / len(split))
        level = level * jnp.repeat(jnp.exp(steps), extent[position] // blocks).reshape((-1,) + (1,) * (len(extent) - 1 - position))
    return level


def scatter_about(stream_key, extent, deviation, reach, pieces=(), kind=jnp.bfloat16):
    level = levels(stream_key, extent, pieces, -0.22, 0.18) if pieces else 1.0
    drawn = jax.random.normal(stream_key, extent, jnp.float32) * deviation * level
    return jnp.minimum(jnp.maximum(drawn, -reach), reach).astype(kind)


def setup_inputs(seed: int = 0) -> dict:
    streams_of = jax.random.split(jax.random.key(seed), 13)
    slab = scatter_about(streams_of[0], (N, SLAB, C), 1.0, 6.0, ((0, 128),))
    pair = scatter_about(streams_of[1], (N, N, C), 1.0, 6.0, ((0, 8), (1, 16)))
    mask = place_ends((jax.random.randint(streams_of[2], (N,), 0, 4) < 3).astype(jnp.int32), jax.random.fold_in(streams_of[2], 1), 0, 1)
    ln_gain = jnp.clip(1.0 + 0.18 * jax.random.normal(streams_of[3], (C,), jnp.float32), 0.1, 1.9)
    w_query = scatter_about(streams_of[4], (C, C), C ** -0.5, 0.5)
    w_key = scatter_about(streams_of[5], (C, C), C ** -0.5, 0.5)
    w_value = scatter_about(streams_of[6], (C, C), C ** -0.5, 0.5)
    w_gate = scatter_about(streams_of[7], (C, C), C ** -0.5, 0.5)
    gate_bias = scatter_about(streams_of[8], (C,), 1.0, 4.0, (), jnp.float32)
    w_bias = draw_w_bias(jax.random.fold_in(streams_of[12], 71), 0)
    w_out = scatter_about(streams_of[10], (C, C), C ** -0.5, 0.5)
    out_bias = scatter_about(streams_of[11], (C,), 0.5, 3.0, (), jnp.float32)
    return dict(slab=slab, pair=pair, mask=mask, ln_gain=ln_gain, w_query=w_query, w_key=w_key, w_value=w_value, w_gate=w_gate, gate_bias=gate_bias, w_bias=w_bias, w_out=w_out, out_bias=out_bias)


def normalize(values, ln_gain):
    values = values.astype(jnp.float32)
    center = lax.optimization_barrier(jnp.mean(values, axis=-1, keepdims=True))
    spread = lax.optimization_barrier(jnp.mean(jnp.square(values - center), axis=-1, keepdims=True))
    return ((values - center) * lax.rsqrt(spread + 1e-05) * ln_gain.astype(jnp.float32)).astype(jnp.bfloat16)

def project(rows, weight):
    flat = rows.reshape(-1, rows.shape[-1])
    result = jnp.dot(flat, weight, preferred_element_type=jnp.float32)
    return result.reshape(rows.shape[:-1] + (weight.shape[1],))

def reference(slab, pair, mask, ln_gain, w_query, w_key, w_value, w_gate, gate_bias, w_bias, w_out, out_bias):
    row_block = math.gcd(N, 32)

    def bias_rows(rows):
        return project(normalize(rows, ln_gain), w_bias).astype(jnp.bfloat16)
    tri_bias = lax.map(bias_rows, pair.reshape(N // row_block, row_block, N, C)).reshape(N, N, H)
    bias_heads = jnp.transpose(tri_bias, (2, 1, 0))
    normed_slab = normalize(slab, ln_gain)
    query = project(normed_slab, w_query).astype(jnp.bfloat16).reshape(N, SLAB, H, DH)
    key = project(normed_slab, w_key).astype(jnp.bfloat16).reshape(N, SLAB, H, DH)
    value = project(normed_slab, w_value).astype(jnp.bfloat16).reshape(N, SLAB, H, DH)
    gate = jax.nn.sigmoid(project(normed_slab, w_gate) + gate_bias)
    key_shift = (mask.astype(jnp.float32) - 1.0) * 1000000000.0
    scale = 1.0 / math.sqrt(DH)

    def column(inputs):
        query_col, key_col, value_col = inputs
        scores = jnp.einsum('ihd,khd->hik', query_col.astype(jnp.float32), key_col.astype(jnp.float32)) * scale
        scores = scores + bias_heads.astype(jnp.float32) + key_shift[None, None, :]
        top = lax.optimization_barrier(jnp.max(scores, axis=-1, keepdims=True))
        weights = jnp.exp(scores - top)
        grouped = weights.reshape(H, N, N_ROW, N_COL, TOK_BLK)
        rounded = grouped.astype(jnp.bfloat16).astype(jnp.float32)
        value_grouped = value_col.reshape(N_ROW, N_COL, TOK_BLK, H, DH).astype(jnp.float32)
        numer_parts = jnp.einsum('hiact,acthd->cihd', rounded, value_grouped)
        denom_parts = lax.optimization_barrier(jnp.sum(grouped, axis=(2, 4)))
        numer = lax.optimization_barrier(jnp.sum(numer_parts.astype(jnp.bfloat16).astype(jnp.float32), axis=0))
        denom = lax.optimization_barrier(jnp.sum(denom_parts.astype(jnp.bfloat16).astype(jnp.float32), axis=2))
        attended = numer / jnp.transpose(denom, (1, 0))[:, :, None]
        return attended.reshape(N, C)
    columns = (jnp.transpose(query, (1, 0, 2, 3)), jnp.transpose(key, (1, 0, 2, 3)), jnp.transpose(value, (1, 0, 2, 3)))
    attended = jnp.transpose(lax.map(column, columns), (1, 0, 2))
    hidden = (gate * attended).astype(jnp.bfloat16)
    update = project(hidden, w_out) + out_bias
    return update.astype(jnp.bfloat16)
```

```python
import functools
import math

import jax
import jax.numpy as jnp
from jax import lax
from jax.experimental import pallas as pl
from jax.experimental.pallas import tpu as pltpu
from jax.sharding import Mesh
from jax.sharding import PartitionSpec as P

F32 = jnp.float32
BF16 = jnp.bfloat16
LOG2E = math.log2(math.e)

AXES = ("x", "zl", "zh", "y", "c")
SIZES = (4, 2, 2, 4, 2)
GROUP = ("x", "zl", "zh")
NG = 16
NB = 8
TB = 8
HEADS = 4
HALF = 4


def layer_norm(x, gain):
    center = jnp.mean(x, axis=-1, keepdims=True)
    d = x - center
    spread = jnp.mean(d * d, axis=-1, keepdims=True)
    return d * lax.rsqrt(spread + 1e-5) * gain


def pack_kernel(slab_ref, pair_ref, gain_ref, wb_ref, out_ref, nslab, npair, rows):
    b = pl.program_id(0)
    gain = gain_ref[...]

    @pl.when(b == 0)
    def _():
        nslab[...] = layer_norm(slab_ref[...].astype(F32).reshape(1024, 128), gain)

    npair[...] = layer_norm(pair_ref[...].astype(F32).reshape(1024, 128), gain)
    wb = wb_ref[...]
    for i in range(TB):
        x = npair[pl.ds(i, 128, stride=TB), :].astype(BF16)
        t = lax.dot_general(wb, x, (((1,), (1,)), ((), ())), preferred_element_type=F32)
        rows[pl.ds(i, TB, stride=TB), :] = t
    bias = rows[0 : HEADS * TB, :].reshape(HEADS, TB, 128).astype(BF16)
    half = (b % 2) * HALF
    for g in range(NG):
        out_ref[g, 0, HALF : HALF + HEADS] = bias
        for j in range(HALF):
            out_ref[g, 0, j] = nslab[pl.ds(half + (g * 8 + j), TB, stride=128), :].astype(BF16)


def attend_kernel(
    idx_ref, recv_ref, other_ref, mask_ref, wkv_ref, wqg_ref, wo_ref, gb_ref, ob_ref,
    out_ref, bias, kbuf, vbuf, qbuf, gate, upd,
):
    b = idx_ref[0]
    core = idx_ref[1]
    for r in range(8):
        shift = (mask_ref[r : r + 1, :].astype(F32) - 1.0) * 1e9
        for h in range(HEADS):
            tile = recv_ref[2 * r : 2 * r + 2, :, HALF + h].astype(F32).reshape(128, 128)
            bias[h * 128 : (h + 1) * 128, r * 128 : (r + 1) * 128] = (tile + shift) * LOG2E

    wkv = wkv_ref[...]
    wqg = wqg_ref[...]
    gb = gb_ref[...]

    def project(src, half):
        def step(j, _):
            col = half * HALF + j
            x = src[:, :, j].astype(F32).reshape(1024, 128).astype(BF16)
            kv = jnp.dot(x, wkv, preferred_element_type=F32)
            kbuf[col] = kv[:, :128].astype(BF16)
            vbuf[col] = kv[:, 128:].astype(BF16)
            xq = src[:, b, j].astype(F32).reshape(128, 128).astype(BF16)
            qg = jnp.dot(xq, wqg, preferred_element_type=F32)
            qbuf[col] = qg[:, :128].astype(BF16)
            gate[col] = jax.nn.sigmoid(qg[:, 128:] + gb)
            return 0

        lax.fori_loop(0, HALF, step, 0)

    project(recv_ref, core)
    project(other_ref, 1 - core)

    lane_head = lax.broadcasted_iota(jnp.int32, (128, 128), 1) // 32
    wo = wo_ref[...]
    ob = ob_ref[...]

    def attend(col, _):
        k = kbuf[col]
        v = vbuf[col]
        q = qbuf[col].astype(F32)
        att = jnp.zeros((128, 128), F32)
        for h in range(HEADS):
            qh = jnp.where(lane_head == h, q, 0.0).astype(BF16)
            s = lax.dot_general(qh, k, (((1,), (1,)), ((), ())), preferred_element_type=F32)
            s = s * (LOG2E / math.sqrt(32.0)) + bias[h * 128 : (h + 1) * 128, :]
            p = jnp.exp2(s - jnp.max(s, axis=-1, keepdims=True))
            total = jnp.sum(p, axis=-1, keepdims=True)
            o = jnp.dot(p.astype(BF16), v, preferred_element_type=F32)
            att = jnp.where(lane_head == h, o * (1.0 / total), att)
        hidden = (gate[col] * att).astype(BF16)
        upd[pl.ds(col, 128, stride=8), :] = jnp.dot(hidden, wo, preferred_element_type=F32) + ob
        return 0

    lax.fori_loop(0, 2 * HALF, attend, 0)
    out_ref[...] = upd[...].reshape(16, 8, 8, 128).astype(BF16)


def pack(slab, pair, gain, wb):
    return pl.pallas_call(
        pack_kernel,
        grid=(NB,),
        in_specs=[
            pl.BlockSpec((8, 128, 128), lambda b: (0, 0, 0)),
            pl.BlockSpec((128, TB, 128), lambda b: (0, b, 0)),
            pl.BlockSpec((1, 128), lambda b: (0, 0)),
            pl.BlockSpec((8, 128), lambda b: (0, 0)),
        ],
        out_specs=pl.BlockSpec((NG, 1, 8, TB, 128), lambda b: (0, b, 0, 0, 0)),
        out_shape=jax.ShapeDtypeStruct((NG, NB, 8, TB, 128), BF16),
        scratch_shapes=[
            pltpu.VMEM((1024, 128), F32),
            pltpu.VMEM((1024, 128), F32),
            pltpu.VMEM((64, 128), F32),
        ],
        name="pack",
    )(slab, pair, gain, wb)


def attend(idx, recv, other, mask, wkv, wqg, wo, gb, ob):
    smem = pl.BlockSpec(memory_space=pltpu.SMEM)
    vmem = pl.BlockSpec(memory_space=pltpu.VMEM)
    return pl.pallas_call(
        attend_kernel,
        in_specs=[smem] + [vmem] * 8,
        out_specs=vmem,
        out_shape=jax.ShapeDtypeStruct((16, TB, 8, 128), BF16),
        scratch_shapes=[
            pltpu.VMEM((512, 1024), F32),
            pltpu.VMEM((8, 1024, 128), BF16),
            pltpu.VMEM((8, 1024, 128), BF16),
            pltpu.VMEM((8, 128, 128), BF16),
            pltpu.VMEM((8, 128, 128), F32),
            pltpu.VMEM((1024, 128), F32),
        ],
        name="attend",
    )(idx, recv, other, mask, wkv, wqg, wo, gb, ob)


def per_device(
    slab, pair, mask, ln_gain, w_query, w_key, w_value, w_gate, gate_bias, w_bias, w_out, out_bias
):
    core = lax.axis_index("c")
    b = lax.axis_index("y") * 2 + core
    wb = jnp.pad(w_bias.T, ((0, 8 - HEADS), (0, 0)))
    packed = pack(slab, pair, ln_gain.reshape(1, 128), wb)
    recv = lax.all_to_all(
        packed.reshape(NG * NB, 8, TB, 128), AXES, split_axis=0, concat_axis=0, tiled=True
    ).reshape(NG, NB, 8, TB, 128)
    other = lax.ppermute(recv[:, :, :HALF], "c", [(0, 1), (1, 0)])
    update = attend(
        jnp.stack([b, core]).astype(jnp.int32),
        recv,
        other,
        mask.reshape(8, 128),
        jnp.concatenate([w_key, w_value], axis=1),
        jnp.concatenate([w_query, w_gate], axis=1),
        w_out,
        gate_bias.reshape(1, 128),
        out_bias.reshape(1, 128),
    )
    home = lax.all_to_all(update, GROUP, split_axis=0, concat_axis=0, tiled=True)
    return jnp.transpose(home, (1, 0, 2, 3)).reshape(8, 128, 128)


def solution(mesh):
    fine = Mesh(mesh.devices.reshape(SIZES), AXES)
    whole = P(AXES, None, None)
    placed = (whole, P(("x", "zl"), ("zh", "y", "c"), None)) + (P(),) * 10
    return jax.shard_map(
        per_device, mesh=fine, in_specs=placed, out_specs=whole, check_vma=False
    )
```

```python
import math

import jax
import jax.numpy as jnp
from jax import lax
from jax.experimental import pallas as pl
from jax.experimental.pallas import tpu as pltpu
from jax.sharding import Mesh
from jax.sharding import PartitionSpec as P

F32 = jnp.float32
BF16 = jnp.bfloat16
LOG2E = math.log2(math.e)

AXES = ("x", "zl", "zh", "y", "c")
SIZES = (4, 2, 2, 4, 2)
GROUP = ("x", "zl", "zh")
NG = 16
NB = 8
TB = 8
HEADS = 4
HALF = 4
COLS = 8
CHUNK = 16

VMEM = pl.BlockSpec(memory_space=pltpu.VMEM)
ANY = pl.BlockSpec(memory_space=pl.ANY)


def pack_kernel(
    slab_ref, pair_ref, gain_ref, wb_ref,
    out_ref, pbuf, nslab, npair, rows, pslab, pbias, in_sem, slab_sem, bias_sem,
):
    loads = [
        pltpu.make_async_copy(pair_ref.at[pl.ds(16 * n, 16)], pbuf.at[pl.ds(16 * n, 16)], in_sem.at[n])
        for n in range(8)
    ]
    for load in loads:
        load.start()
    ones = jnp.full((128, 128), 1.0 / 128, BF16)
    gain = gain_ref[...]
    wb = wb_ref[...]

    def norm(x):
        d = x.astype(F32) - jnp.dot(x, ones, preferred_element_type=F32)
        spread = jnp.mean(d * d, axis=-1, keepdims=True)
        return d * lax.rsqrt(spread + 1e-5) * gain

    nslab[...] = norm(slab_ref[...].reshape(1024, 128))
    for col in range(128):
        piece = nslab[pl.ds(col, TB, stride=128), :].astype(BF16)
        pslab[col // COLS, col % COLS // HALF, col % HALF] = piece
    stores = [
        pltpu.make_async_copy(pslab, out_ref.at[:, pl.ds(2 * y, 2), pl.ds(0, HALF)], slab_sem.at[y])
        for y in range(4)
    ]
    for store in stores:
        store.start()
    for n in range(8):
        loads[n].wait()
        x = norm(pbuf[16 * n : 16 * n + 16].reshape(1024, 128))
        for k in range(16):
            for b in range(NB):
                at = 1024 * b + TB * (16 * n + k)
                npair[at : at + TB, :] = x[64 * k + TB * b : 64 * k + TB * b + TB]
    for b in range(NB):
        for i in range(TB):
            x = npair[pl.ds(1024 * b + i, 128, stride=TB), :].astype(BF16)
            t = lax.dot_general(wb, x, (((1,), (1,)), ((), ())), preferred_element_type=F32)
            rows[pl.ds(HEADS * TB * b + i, HEADS, stride=TB), :] = t
    pbias[...] = rows[...].reshape(NB, HEADS, TB, 128).astype(BF16)
    more = [
        pltpu.make_async_copy(pbias, out_ref.at[g, :, pl.ds(HALF, HEADS)], bias_sem.at[g])
        for g in range(NG)
    ]
    for store in more:
        store.start()
    for store in stores + more:
        store.wait()


def pack(slab, pair, gain, wb):
    return pl.pallas_call(
        pack_kernel,
        in_specs=[VMEM, ANY, VMEM, VMEM],
        out_specs=ANY,
        out_shape=jax.ShapeDtypeStruct((NG, NB, HALF + HEADS, TB, 128), BF16),
        scratch_shapes=[
            pltpu.VMEM((128, 64, 128), BF16),
            pltpu.VMEM((1024, 128), F32),
            pltpu.VMEM((8192, 128), F32),
            pltpu.VMEM((NB * HEADS * TB, 128), F32),
            pltpu.VMEM((NG, 2, HALF, TB, 128), BF16),
            pltpu.VMEM((NB, HEADS, TB, 128), BF16),
            pltpu.SemaphoreType.DMA((8,)),
            pltpu.SemaphoreType.DMA((4,)),
            pltpu.SemaphoreType.DMA((NG,)),
        ],
        name="pack",
    )(slab, pair, gain, wb)


def attend_kernel(
    own_ref, other_ref, tiles_ref, mask_ref, wk_ref, wv_ref, wq_ref, wg_ref, gb_ref, wo_ref, ob_ref,
    out_ref, bias, s_even, s_odd, v_even, v_odd, g_even, g_odd, weights, inverse, product, upd,
):
    step = pl.program_id(0)
    core = lax.axis_index("c")
    b = 2 * lax.axis_index("y") + core

    @pl.when(step == 0)
    def _():
        for r in range(8):
            shift = (mask_ref[r : r + 1, :].astype(F32) - 1.0) * 1e9
            for h in range(HEADS):
                tile = tiles_ref[2 * r : 2 * r + 2, :, h].astype(F32).reshape(128, 128)
                bias[h * 128 : (h + 1) * 128, r * 128 : (r + 1) * 128] = (tile + shift) * LOG2E

    lane_head = lax.broadcasted_iota(jnp.int32, (128, 128), 1) // 32
    mine = step < HALF

    def pick(own, other):
        return jnp.where(mine, own.astype(F32), other.astype(F32))

    def queries(gate):
        xq = pick(own_ref[:, b, 0], other_ref[:, b, 0]).reshape(128, 128).astype(BF16)
        wqg = jnp.concatenate([wq_ref[...], wg_ref[...]], axis=1)
        qg = jnp.dot(xq, wqg, preferred_element_type=F32)
        gate[...] = jax.nn.sigmoid(qg[:, 128:] + gb_ref[...])
        q = qg[:, :128].astype(BF16).astype(F32)
        return jnp.concatenate(
            [jnp.where(lane_head == h, q, 0.0).astype(BF16) for h in range(HEADS)], axis=0
        )

    def scores(n, q, new, value):
        at = slice(n * 4, n * 4 + 4)
        keys = slice(n * 256, n * 256 + 256)
        x = pick(own_ref[at, :, 0], other_ref[at, :, 0]).reshape(256, 128).astype(BF16)
        wkv = jnp.concatenate([wk_ref[...], wv_ref[...]], axis=1)
        kv = jnp.dot(x, wkv, preferred_element_type=F32)
        value[keys, :] = kv[:, 128:].astype(BF16)
        s = lax.dot_general(
            q, kv[:, :128].astype(BF16), (((1,), (1,)), ((), ())), preferred_element_type=F32
        )
        new[:, keys] = s * (LOG2E / math.sqrt(32.0)) + bias[:, keys]

    def softmax(n, old):
        for m in range(n * 128, n * 128 + 128, CHUNK):
            at = slice(m, m + CHUNK)
            s = old[at, :]
            p = jnp.exp2(s - jnp.max(s, axis=-1, keepdims=True))
            total = jnp.sum(p, axis=-1, keepdims=True)
            weights[at, :] = p.astype(BF16)
            inverse[at, :] = jnp.broadcast_to(1.0 / total, (CHUNK, 128))

    def products(n, value):
        at = slice(n * 256, n * 256 + 256)
        o = jnp.dot(weights[at, :], value[...], preferred_element_type=F32)
        product[at, :] = o * inverse[at, :]

    def finish(gate):
        att = product[0:128]
        for h in range(1, HEADS):
            att = jnp.where(lane_head == h, product[h * 128 : (h + 1) * 128], att)
        hidden = (gate[...] * att).astype(BF16)
        u = jnp.dot(hidden, wo_ref[...], preferred_element_type=F32) + ob_ref[...]
        before = step - 1
        col = jnp.where(before < HALF, before + core * HALF, before - core * HALF)
        upd[pl.ds(col, 128, stride=COLS), :] = u

    def body(new, old):
        if new is not None:
            q = queries(new[2])
        for n in range(4):
            if new is not None:
                scores(n, q, new[0], new[1])
            if old is not None:
                softmax(n, old[0])
                if n % 2:
                    products(n // 2, old[1])
        if old is not None:
            finish(old[2])

    even = (s_even, v_even, g_even)
    odd = (s_odd, v_odd, g_odd)

    @pl.when(step == 0)
    def _():
        body(even, None)

    @pl.when((step % 2 == 0) & (step > 0) & (step < COLS))
    def _():
        body(even, odd)

    @pl.when(step % 2 == 1)
    def _():
        body(odd, even)

    @pl.when(step == COLS)
    def _():
        body(None, odd)
        out_ref[...] = upd[...].reshape(16, TB, COLS, 128).astype(BF16)


def attend(recv, other, mask, wk, wv, wq, wg, gb, wo, ob):
    const = lambda s: (0, 0)
    column = (NG, NB, 1, TB, 128)
    square = pl.BlockSpec((128, 128), const)
    line = pl.BlockSpec((1, 128), const)
    return pl.pallas_call(
        attend_kernel,
        grid=(COLS + 1,),
        in_specs=[
            pl.BlockSpec(column, lambda s: (0, 0, jnp.minimum(s, HALF - 1), 0, 0)),
            pl.BlockSpec(column, lambda s: (0, 0, jnp.clip(s - HALF, 0, HALF - 1), 0, 0)),
            pl.BlockSpec((NG, NB, HEADS, TB, 128), lambda s: (0, 0, 1, 0, 0)),
            pl.BlockSpec((8, 128), const),
            square,
            square,
            square,
            square,
            line,
            square,
            line,
        ],
        out_specs=pl.BlockSpec((NG, TB, COLS, 128), lambda s: (0, 0, 0, 0)),
        out_shape=jax.ShapeDtypeStruct((NG, TB, COLS, 128), BF16),
        scratch_shapes=[
            pltpu.VMEM((512, 1024), F32),
            pltpu.VMEM((512, 1024), F32),
            pltpu.VMEM((512, 1024), F32),
            pltpu.VMEM((1024, 128), BF16),
            pltpu.VMEM((1024, 128), BF16),
            pltpu.VMEM((128, 128), F32),
            pltpu.VMEM((128, 128), F32),
            pltpu.VMEM((512, 1024), BF16),
            pltpu.VMEM((512, 128), F32),
            pltpu.VMEM((512, 128), F32),
            pltpu.VMEM((1024, 128), F32),
        ],
        name="attend",
    )(recv, other, recv, mask, wk, wv, wq, wg, gb, wo, ob)


def per_device(
    slab, pair, mask, ln_gain, w_query, w_key, w_value, w_gate, gate_bias, w_bias, w_out, out_bias
):
    packed = pack(slab, pair, ln_gain.reshape(1, 128), w_bias.T)
    recv = lax.all_to_all(
        packed.reshape(NG * NB, HALF + HEADS, TB, 128), AXES, split_axis=0, concat_axis=0, tiled=True
    ).reshape(packed.shape)
    other = lax.ppermute(recv[:, :, :HALF], "c", [(0, 1), (1, 0)])
    update = attend(
        recv, other, mask.reshape(8, 128), w_key, w_value, w_query, w_gate,
        gate_bias.reshape(1, 128), w_out, out_bias.reshape(1, 128),
    )
    home = lax.all_to_all(update, GROUP, split_axis=0, concat_axis=0, tiled=True)
    return jnp.transpose(home, (1, 0, 2, 3)).reshape(8, 128, 128)


def solution(mesh):
    fine = Mesh(mesh.devices.reshape(SIZES), AXES)
    whole = P(AXES, None, None)
    placed = (whole, P(("x", "zl"), ("zh", "y", "c"), None)) + (P(),) * 10
    return jax.shard_map(
        per_device, mesh=fine, in_specs=placed, out_specs=whole, check_vma=False
    )
```

```python
import math

import jax
import jax.numpy as jnp
from jax import lax
from jax.experimental import pallas as pl
from jax.experimental.pallas import tpu as pltpu
from jax.sharding import Mesh
from jax.sharding import PartitionSpec as P

F32 = jnp.float32
BF16 = jnp.bfloat16
LOG2E = math.log2(math.e)

AXES = ("x", "zl", "zh", "y", "c")
SIZES = (4, 2, 2, 4, 2)
GROUP = ("x", "zl", "zh")
NG = 16
NB = 8
TB = 8
HEADS = 4
HALF = 4
COLS = 8
CHUNK = 16

VMEM = pl.BlockSpec(memory_space=pltpu.VMEM)
HBM = pl.BlockSpec(memory_space=pltpu.HBM)


def pack_kernel(
    slab_ref, pair_ref, gain_hbm, wb_hbm, out_ref, pbuf, sbuf, gain_ref, wb_ref, nslab, npair, rows, in_sem
):
    loads = [
        pltpu.make_async_copy(pair_ref.at[pl.ds(16 * n, 16)], pbuf.at[pl.ds(16 * n, 16)], in_sem.at[n])
        for n in range(8)
    ]
    gain_load = pltpu.make_async_copy(gain_hbm, gain_ref, in_sem.at[8])
    wb_load = pltpu.make_async_copy(wb_hbm, wb_ref, in_sem.at[9])
    slab_load = pltpu.make_async_copy(slab_ref, sbuf, in_sem.at[10])
    gain_load.start()
    for load in loads:
        load.start()
    wb_load.start()
    slab_load.start()
    gain_load.wait()
    ones = jnp.full((128, 128), 1.0 / 128, BF16)
    gain = gain_ref[...]

    def norm(x):
        d = x.astype(F32) - jnp.dot(x, ones, preferred_element_type=F32)
        spread = jnp.mean(d * d, axis=-1, keepdims=True)
        return d * lax.rsqrt(spread + 1e-5) * gain

    for n in range(8):
        loads[n].wait()
        x = norm(pbuf[16 * n : 16 * n + 16].reshape(1024, 128))
        for k in range(16):
            for b in range(NB):
                at = 1024 * b + TB * (16 * n + k)
                npair[at : at + TB, :] = x[64 * k + TB * b : 64 * k + TB * b + TB]
    wb_load.wait()
    wb = wb_ref[...]
    slab_load.wait()
    nslab[...] = norm(sbuf[...].reshape(1024, 128))
    for b in range(NB):
        for i in range(TB):
            x = npair[pl.ds(1024 * b + i, 128, stride=TB), :].astype(BF16)
            t = lax.dot_general(wb, x, (((1,), (1,)), ((), ())), preferred_element_type=F32)
            rows[pl.ds(HEADS * TB * b + i, HEADS, stride=TB), :] = t
        at = slice(HEADS * TB * b, HEADS * TB * b + HEADS * TB)
        bias = rows[at, :].reshape(HEADS, TB, 128).astype(BF16)
        for g in range(NG):
            out_ref[g, b, HALF : HALF + HEADS] = bias
    for col in range(128):
        piece = nslab[pl.ds(col, TB, stride=128), :].astype(BF16)
        for y in range(4):
            out_ref[col // COLS, 2 * y + col % COLS // HALF, col % HALF] = piece


def pack(slab, pair, gain, wb):
    return pl.pallas_call(
        pack_kernel,
        in_specs=[HBM] * 4,
        out_specs=VMEM,
        out_shape=jax.ShapeDtypeStruct((NG, NB, HALF + HEADS, TB, 128), BF16),
        scratch_shapes=[
            pltpu.VMEM((128, 64, 128), BF16),
            pltpu.VMEM((8, 128, 128), BF16),
            pltpu.VMEM((1, 128), F32),
            pltpu.VMEM((HEADS, 128), BF16),
            pltpu.VMEM((1024, 128), F32),
            pltpu.VMEM((8192, 128), F32),
            pltpu.VMEM((NB * HEADS * TB + 64, 128), F32),
            pltpu.SemaphoreType.DMA((11,)),
        ],
        compiler_params=pltpu.CompilerParams(vmem_limit_bytes=30 << 20),
        name="pack",
    )(*(pltpu.with_memory_space_constraint(a, pltpu.HBM) for a in (slab, pair, gain, wb)))


def attend_kernel(
    recv_ref, other_ref, mask_ref, wk_ref, wv_ref, wq_ref, wg_ref, gb_ref, wo_ref, ob_ref,
    out_ref, bias, s_even, s_odd, v_even, v_odd, g_even, g_odd, weights, inverse, product, upd,
):
    step = pl.program_id(0)
    core = lax.axis_index("c")
    b = 2 * lax.axis_index("y") + core

    @pl.when(step == 0)
    def _():
        for r in range(8):
            shift = (mask_ref[r : r + 1, :].astype(F32) - 1.0) * 1e9
            for h in range(HEADS):
                tile = recv_ref[2 * r : 2 * r + 2, :, HALF + h].astype(F32).reshape(128, 128)
                bias[h * 128 : (h + 1) * 128, r * 128 : (r + 1) * 128] = (tile + shift) * LOG2E

    lane_head = lax.broadcasted_iota(jnp.int32, (128, 128), 1) // 32
    mine = step < HALF
    j_own = jnp.minimum(step, HALF - 1)
    j_other = jnp.clip(step - HALF, 0, HALF - 1)

    def pick(own, other):
        return jnp.where(mine, own.astype(F32), other.astype(F32))

    def queries(gate):
        xq = pick(recv_ref[:, b, j_own], other_ref[:, b, j_other]).reshape(128, 128).astype(BF16)
        wqg = jnp.concatenate([wq_ref[...], wg_ref[...]], axis=1)
        qg = jnp.dot(xq, wqg, preferred_element_type=F32)
        gate[...] = jax.nn.sigmoid(qg[:, 128:] + gb_ref[...])
        q = qg[:, :128].astype(BF16).astype(F32)
        return jnp.concatenate(
            [jnp.where(lane_head == h, q, 0.0).astype(BF16) for h in range(HEADS)], axis=0
        )

    def scores(n, q, new, value):
        at = slice(n * 4, n * 4 + 4)
        keys = slice(n * 256, n * 256 + 256)
        x = pick(recv_ref[at, :, j_own], other_ref[at, :, j_other]).reshape(256, 128).astype(BF16)
        wkv = jnp.concatenate([wk_ref[...], wv_ref[...]], axis=1)
        kv = jnp.dot(x, wkv, preferred_element_type=F32)
        value[keys, :] = kv[:, 128:].astype(BF16)
        s = lax.dot_general(
            q, kv[:, :128].astype(BF16), (((1,), (1,)), ((), ())), preferred_element_type=F32
        )
        new[:, keys] = s * (LOG2E / math.sqrt(32.0)) + bias[:, keys]

    def softmax(n, old):
        for m in range(n * 128, n * 128 + 128, CHUNK):
            at = slice(m, m + CHUNK)
            s = old[at, :]
            p = jnp.exp2(s - jnp.max(s, axis=-1, keepdims=True))
            total = jnp.sum(p, axis=-1, keepdims=True)
            weights[at, :] = p.astype(BF16)
            inverse[at, :] = jnp.broadcast_to(1.0 / total, (CHUNK, 128))

    def products(n, value):
        at = slice(n * 256, n * 256 + 256)
        o = jnp.dot(weights[at, :], value[...], preferred_element_type=F32)
        product[at, :] = o * inverse[at, :]

    def finish(gate):
        att = product[0:128]
        for h in range(1, HEADS):
            att = jnp.where(lane_head == h, product[h * 128 : (h + 1) * 128], att)
        hidden = (gate[...] * att).astype(BF16)
        u = jnp.dot(hidden, wo_ref[...], preferred_element_type=F32) + ob_ref[...]
        before = step - 1
        col = jnp.where(before < HALF, before + core * HALF, before - core * HALF)
        upd[pl.ds(col, 128, stride=COLS), :] = u

    def body(new, old):
        if new is not None:
            q = queries(new[2])
        for n in range(4):
            if new is not None:
                scores(n, q, new[0], new[1])
            if old is not None:
                softmax(n, old[0])
                if n % 2:
                    products(n // 2, old[1])
        if old is not None:
            finish(old[2])

    even = (s_even, v_even, g_even)
    odd = (s_odd, v_odd, g_odd)

    @pl.when(step == 0)
    def _():
        body(even, None)

    @pl.when((step % 2 == 0) & (step > 0) & (step < COLS))
    def _():
        body(even, odd)

    @pl.when(step % 2 == 1)
    def _():
        body(odd, even)

    @pl.when(step == COLS)
    def _():
        body(None, odd)
        out_ref[...] = upd[...].reshape(16, TB, COLS, 128).astype(BF16)


def attend(recv, other, mask, wk, wv, wq, wg, gb, wo, ob):
    const = lambda s: (0, 0)
    column = (NG, NB, 1, TB, 128)
    square = pl.BlockSpec((128, 128), const)
    line = pl.BlockSpec((1, 128), const)
    return pl.pallas_call(
        attend_kernel,
        grid=(COLS + 1,),
        in_specs=[
            VMEM,
            VMEM,
            pl.BlockSpec((8, 128), const),
            square,
            square,
            square,
            square,
            line,
            square,
            line,
        ],
        out_specs=pl.BlockSpec((NG, TB, COLS, 128), lambda s: (0, 0, 0, 0)),
        out_shape=jax.ShapeDtypeStruct((NG, TB, COLS, 128), BF16),
        scratch_shapes=[
            pltpu.VMEM((512, 1024), F32),
            pltpu.VMEM((512, 1024), F32),
            pltpu.VMEM((512, 1024), F32),
            pltpu.VMEM((1024, 128), BF16),
            pltpu.VMEM((1024, 128), BF16),
            pltpu.VMEM((128, 128), F32),
            pltpu.VMEM((128, 128), F32),
            pltpu.VMEM((512, 1024), BF16),
            pltpu.VMEM((512, 128), F32),
            pltpu.VMEM((512, 128), F32),
            pltpu.VMEM((1024, 128), F32),
        ],
        compiler_params=pltpu.CompilerParams(vmem_limit_bytes=40 << 20),
        name="attend",
    )(
        pltpu.with_memory_space_constraint(recv, pltpu.VMEM),
        pltpu.with_memory_space_constraint(other, pltpu.VMEM),
        mask, wk, wv, wq, wg, gb, wo, ob)


def per_device(
    slab, pair, mask, ln_gain, w_query, w_key, w_value, w_gate, gate_bias, w_bias, w_out, out_bias
):
    packed = pack(slab, pair, ln_gain.reshape(1, 128), w_bias.T)
    recv = lax.all_to_all(
        packed.reshape(NG * NB, HALF + HEADS, TB, 128), AXES, split_axis=0, concat_axis=0, tiled=True
    ).reshape(packed.shape)
    other = lax.ppermute(recv[:, :, :HALF], "c", [(0, 1), (1, 0)])
    update = attend(
        recv, other, mask.reshape(8, 128), w_key, w_value, w_query, w_gate,
        gate_bias.reshape(1, 128), w_out, out_bias.reshape(1, 128),
    )
    home = lax.all_to_all(update, GROUP, split_axis=0, concat_axis=0, tiled=True)
    return jnp.transpose(home, (1, 0, 2, 3)).reshape(8, 128, 128)


def solution(mesh):
    fine = Mesh(mesh.devices.reshape(SIZES), AXES)
    whole = P(AXES, None, None)
    placed = (whole, P(("x", "zl"), ("zh", "y", "c"), None)) + (P(),) * 10
    return jax.shard_map(
        per_device, mesh=fine, in_specs=placed, out_specs=whole, check_vma=False
    )
```

```python
import math

import jax
import jax.numpy as jnp
from jax import lax
from jax.experimental import pallas as pl
from jax.experimental.pallas import tpu as pltpu
from jax.sharding import Mesh
from jax.sharding import PartitionSpec as P

F32 = jnp.float32
BF16 = jnp.bfloat16
LOG2E = math.log2(math.e)

AXES = ("x", "zl", "zh", "y", "c")
SIZES = (4, 2, 2, 4, 2)
GROUP = ("x", "zl", "zh")
NG = 16
NB = 8
TB = 8
HEADS = 4
HALF = 4
COLS = 8
CHUNK = 16

VMEM = pl.BlockSpec(memory_space=pltpu.VMEM)
HBM = pl.BlockSpec(memory_space=pltpu.HBM)


def pack_kernel(
    slab_ref, pair_ref, gain_hbm, wb_hbm, out_ref, pbuf, sbuf, gain_ref, wb_ref, nslab, npair, rows, in_sem
):
    loads = [
        pltpu.make_async_copy(pair_ref.at[pl.ds(16 * n, 16)], pbuf.at[pl.ds(16 * n, 16)], in_sem.at[n])
        for n in range(8)
    ]
    gain_load = pltpu.make_async_copy(gain_hbm, gain_ref, in_sem.at[8])
    wb_load = pltpu.make_async_copy(wb_hbm, wb_ref, in_sem.at[9])
    slab_load = pltpu.make_async_copy(slab_ref, sbuf, in_sem.at[10])
    gain_load.start()
    for load in loads:
        load.start()
    wb_load.start()
    slab_load.start()
    gain_load.wait()
    ones = jnp.full((128, 128), 1.0 / 128, BF16)
    gain = gain_ref[...]

    def norm(x):
        d = x.astype(F32) - jnp.dot(x, ones, preferred_element_type=F32)
        spread = jnp.mean(d * d, axis=-1, keepdims=True)
        return d * lax.rsqrt(spread + 1e-5) * gain

    for n in range(8):
        loads[n].wait()
        x = norm(pbuf[16 * n : 16 * n + 16].reshape(1024, 128))
        for k in range(16):
            for b in range(NB):
                at = 1024 * b + TB * (16 * n + k)
                npair[at : at + TB, :] = x[64 * k + TB * b : 64 * k + TB * b + TB]
    wb_load.wait()
    wb = wb_ref[...]
    slab_load.wait()
    nslab[...] = norm(sbuf[...].reshape(1024, 128))
    for b in range(NB):
        for i in range(TB):
            x = npair[pl.ds(1024 * b + i, 128, stride=TB), :].astype(BF16)
            t = lax.dot_general(wb, x, (((1,), (1,)), ((), ())), preferred_element_type=F32)
            rows[pl.ds(HEADS * TB * b + i, HEADS, stride=TB), :] = t
        at = slice(HEADS * TB * b, HEADS * TB * b + HEADS * TB)
        bias = rows[at, :].reshape(HEADS, TB, 128).astype(BF16)
        for g in range(NG):
            out_ref[g, b, HALF : HALF + HEADS] = bias
    for col in range(128):
        piece = nslab[pl.ds(col, TB, stride=128), :].astype(BF16)
        for y in range(4):
            out_ref[col // COLS, 2 * y + col % COLS // HALF, col % HALF] = piece


def pack(slab, pair, gain, wb):
    return pl.pallas_call(
        pack_kernel,
        in_specs=[HBM] * 4,
        out_specs=VMEM,
        out_shape=jax.ShapeDtypeStruct((NG, NB, HALF + HEADS, TB, 128), BF16),
        scratch_shapes=[
            pltpu.VMEM((128, 64, 128), BF16),
            pltpu.VMEM((8, 128, 128), BF16),
            pltpu.VMEM((1, 128), F32),
            pltpu.VMEM((HEADS, 128), BF16),
            pltpu.VMEM((1024, 128), F32),
            pltpu.VMEM((8192, 128), F32),
            pltpu.VMEM((NB * HEADS * TB + 64, 128), F32),
            pltpu.SemaphoreType.DMA((11,)),
        ],
        compiler_params=pltpu.CompilerParams(vmem_limit_bytes=30 << 20),
        name="pack",
    )(*(pltpu.with_memory_space_constraint(a, pltpu.HBM) for a in (slab, pair, gain, wb)))


def attend_kernel(
    recv_ref, other_ref, mask_ref, wk_ref, wv_ref, wq_ref, wg_ref, gb_ref, wo_ref, ob_ref,
    out_ref, bias, s_even, s_odd, v_even, v_odd, g_even, g_odd, weights, product, upd,
):
    step = pl.program_id(0)
    core = lax.axis_index("c")
    b = 2 * lax.axis_index("y") + core

    @pl.when(step == 0)
    def _():
        for r in range(8):
            shift = (mask_ref[r : r + 1, :].astype(F32) - 1.0) * 1e9
            for h in range(HEADS):
                tile = recv_ref[2 * r : 2 * r + 2, :, HALF + h].astype(F32).reshape(128, 128)
                bias[h * 128 : (h + 1) * 128, r * 128 : (r + 1) * 128] = (tile + shift) * LOG2E

    lane_head = lax.broadcasted_iota(jnp.int32, (128, 128), 1) // 32

    def queries(source, gate):
        ref, j = source
        xq = ref[:, b, j].astype(F32).reshape(128, 128).astype(BF16)
        wqg = jnp.concatenate([wq_ref[...], wg_ref[...]], axis=1)
        qg = jnp.dot(xq, wqg, preferred_element_type=F32)
        gate[...] = jax.nn.sigmoid(qg[:, 128:] + gb_ref[...])
        q = qg[:, :128].astype(BF16).astype(F32)
        return jnp.concatenate(
            [jnp.where(lane_head == h, q, 0.0).astype(BF16) for h in range(HEADS)], axis=0
        )

    def scores(n, source, q, new, value):
        ref, j = source
        at = slice(n * 4, n * 4 + 4)
        keys = slice(n * 256, n * 256 + 256)
        x = ref[at, :, j].astype(F32).reshape(256, 128).astype(BF16)
        wkv = jnp.concatenate([wk_ref[...], wv_ref[...]], axis=1)
        kv = jnp.dot(x, wkv, preferred_element_type=F32)
        value[keys, :128] = kv[:, 128:].astype(BF16)
        s = lax.dot_general(
            q, kv[:, :128].astype(BF16), (((1,), (1,)), ((), ())), preferred_element_type=F32
        )
        new[:, keys] = s * (LOG2E / math.sqrt(32.0)) + bias[:, keys]

    def softmax(n, old):
        for m in range(n * 128, n * 128 + 128, CHUNK):
            at = slice(m, m + CHUNK)
            s = old[at, :]
            p = jnp.exp2(s - jnp.max(s, axis=-1, keepdims=True))
            weights[at, :] = p.astype(BF16)

    def products(n, value):
        at = slice(n * 256, n * 256 + 256)
        o = jnp.dot(weights[at, :], value[...], preferred_element_type=F32)
        product[at, :] = o[:, :128] * (1.0 / o[:, 128:])

    def finish(gate):
        att = product[0:128]
        for h in range(1, HEADS):
            att = jnp.where(lane_head == h, product[h * 128 : (h + 1) * 128], att)
        hidden = (gate[...] * att).astype(BF16)
        u = jnp.dot(hidden, wo_ref[...], preferred_element_type=F32) + ob_ref[...]
        before = step - 1
        col = jnp.where(before < HALF, before + core * HALF, before - core * HALF)
        upd[pl.ds(col, 128, stride=COLS), :] = u

    def body(source, new, old):
        if new is not None:
            q = queries(source, new[2])
        for n in range(4):
            if new is not None:
                scores(n, source, q, new[0], new[1])
            if old is not None:
                softmax(n, old[0])
                if n % 2:
                    products(n // 2, old[1])
        if old is not None:
            finish(old[2])

    even = (s_even, v_even, g_even)
    odd = (s_odd, v_odd, g_odd)

    @pl.when(step == 0)
    def _():
        v_even[:, 128:] = jnp.ones((1024, 128), BF16)
        v_odd[:, 128:] = jnp.ones((1024, 128), BF16)
        body((recv_ref, 0), even, None)

    own = (recv_ref, jnp.minimum(step, HALF - 1))
    other = (other_ref, jnp.clip(step - HALF, 0, HALF - 1))
    for source, here in ((own, (step > 0) & (step < HALF)), (other, (step >= HALF) & (step < COLS))):

        @pl.when(here & (step % 2 == 0))
        def _(source=source):
            body(source, even, odd)

        @pl.when(here & (step % 2 == 1))
        def _(source=source):
            body(source, odd, even)

    @pl.when(step == COLS)
    def _():
        body(None, None, odd)
        out_ref[...] = upd[...].reshape(16, TB, COLS, 128).astype(BF16)


def attend(recv, other, mask, wk, wv, wq, wg, gb, wo, ob):
    const = lambda s: (0, 0)
    column = (NG, NB, 1, TB, 128)
    square = pl.BlockSpec((128, 128), const)
    line = pl.BlockSpec((1, 128), const)
    return pl.pallas_call(
        attend_kernel,
        grid=(COLS + 1,),
        in_specs=[
            VMEM,
            VMEM,
            pl.BlockSpec((8, 128), const),
            square,
            square,
            square,
            square,
            line,
            square,
            line,
        ],
        out_specs=pl.BlockSpec((NG, TB, COLS, 128), lambda s: (0, 0, 0, 0)),
        out_shape=jax.ShapeDtypeStruct((NG, TB, COLS, 128), BF16),
        scratch_shapes=[
            pltpu.VMEM((512, 1024), F32),
            pltpu.VMEM((512, 1024), F32),
            pltpu.VMEM((512, 1024), F32),
            pltpu.VMEM((1024, 256), BF16),
            pltpu.VMEM((1024, 256), BF16),
            pltpu.VMEM((128, 128), F32),
            pltpu.VMEM((128, 128), F32),
            pltpu.VMEM((512, 1024), BF16),
            pltpu.VMEM((512, 128), F32),
            pltpu.VMEM((1024, 128), F32),
        ],
        compiler_params=pltpu.CompilerParams(vmem_limit_bytes=40 << 20),
        name="attend",
    )(
        pltpu.with_memory_space_constraint(recv, pltpu.VMEM),
        pltpu.with_memory_space_constraint(other, pltpu.VMEM),
        mask, wk, wv, wq, wg, gb, wo, ob)


def per_device(
    slab, pair, mask, ln_gain, w_query, w_key, w_value, w_gate, gate_bias, w_bias, w_out, out_bias
):
    packed = pack(slab, pair, ln_gain.reshape(1, 128), w_bias.T)
    recv = lax.all_to_all(
        packed.reshape(NG * NB, HALF + HEADS, TB, 128), AXES, split_axis=0, concat_axis=0, tiled=True
    ).reshape(packed.shape)
    other = lax.ppermute(recv[:, :, :HALF], "c", [(0, 1), (1, 0)])
    update = attend(
        recv, other, mask.reshape(8, 128), w_key, w_value, w_query, w_gate,
        gate_bias.reshape(1, 128), w_out, out_bias.reshape(1, 128),
    )
    home = lax.all_to_all(update, GROUP, split_axis=0, concat_axis=0, tiled=True)
    return jnp.transpose(home, (1, 0, 2, 3)).reshape(8, 128, 128)


def solution(mesh):
    fine = Mesh(mesh.devices.reshape(SIZES), AXES)
    whole = P(AXES, None, None)
    placed = (whole, P(("x", "zl"), ("zh", "y", "c"), None)) + (P(),) * 10
    return jax.shard_map(
        per_device, mesh=fine, in_specs=placed, out_specs=whole, check_vma=False
    )
```
